32 devices in a mesh: tm: 4 (over y, x), space: 8 (over z, core).
Axes of the slice: x: 2, y: 2, z: 4, core: 2. Of those that a mesh axis runs over, the one named last changes fastest.
Arguments:
- states: float32 [4, 256, 256, 256], P('tm', 'space'), may hold values from -4 to 4
- forcing: float32 [4, 256, 256, 256], P('tm', 'space'), may hold values from -4 to 4
- inflow: float32 [256, 256, 256], P('space'), may hold values from -4 to 4
- timestep: float32 [1], replicated, may hold values from 0.05 to 0.2
Outputs:
- new_states: float32 [4, 256, 256, 256], P('tm', 'space')
- defects: float32 [4, 256, 256, 256], P('tm', 'space')
The draws below stay inside these ranges and needn't reach their ends.
All inputs are finite; a program needn't handle non-finite values.
Results may differ from the reference program's by a relative error of at most 0.00013.
Values sent between devices are 32-bit elements; how exact they have to be, the bound alone decides.
A program may use at most 192 MiB of HBM per device.

```python
import math
import jax
import jax.numpy as jnp

GRID = 256
FINE = 8
INTERVALS = 4


def draw_forcing(key, part):
    extents = (INTERVALS, GRID, GRID, GRID)
    jagged = jax.random.normal(key, extents, jnp.float32)
    return jnp.clip(jagged, -4.0, 4.0)


def levels(rng, extent, cuts, smallest, largest):
    gain = 1.0
    for dim, blocks in cuts:
        steps = jax.random.uniform(jax.random.fold_in(jax.random.fold_in(rng, 6), dim), (blocks,), jnp.float32, smallest / len(cuts), largest / len(cuts))
        gain = gain * jnp.repeat(jnp.exp(steps), extent[dim] // blocks).reshape((-1,) + (1,) * (len(extent) - 1 - dim))
    return gain


def gaussian(own_key, extent, scale, most, split=(), kind=jnp.bfloat16):
    drawn = jax.random.normal(own_key, extent, jnp.float32) * scale
    if len(split) > 0:
        drawn = levels(own_key, extent, split, -0.22, 0.18) * drawn
    return jnp.clip(drawn, min=-most, max=most).astype(kind)


def setup_inputs(seed: int = 0) -> dict:
    key_list = jax.random.split(jax.random.key(seed), 5)
    states = gaussian(key_list[0], (INTERVALS, GRID, GRID, GRID), 1.0, 4.0, ((0, 4), (1, 8)), jnp.float32)
    forcing = draw_forcing(jax.random.fold_in(key_list[4], 71), 0)
    inflow = gaussian(key_list[2], (GRID, GRID, GRID), 1.0, 4.0, ((0, 8),), jnp.float32)
    timestep = jnp.clip(jnp.exp(jax.random.uniform(key_list[3], (1,), jnp.float32, math.log(0.05), math.log(0.2))), 0.05, 0.2)
    return dict(states=states, forcing=forcing, inflow=inflow, timestep=timestep)


def symbols(stepsize):
    angles = jnp.arange(GRID, dtype=jnp.float32) * (2.0 * math.pi / GRID)
    lattice = 2.0 - 2.0 * jnp.cos(angles)
    laplace = lattice[:, None, None] + lattice[None, :, None] + lattice[None, None, : GRID // 2 + 1]
    damping = 1.0 / (1.0 + stepsize * laplace)
    coarse = 1.0 / (1.0 + FINE * stepsize * laplace)
    return damping, coarse


def reference(states, forcing, inflow, timestep):
    stepsize = timestep[0]
    damping, coarse = symbols(stepsize)
    spec_states = jnp.fft.rfftn(states, axes=(1, 2, 3))
    spec_forcing = jnp.fft.rfftn(forcing, axes=(1, 2, 3))
    spec_inflow = jnp.fft.rfftn(inflow)

    def advance(spectrum, source):
        for repeat in range(FINE):
            spectrum = damping * (spectrum + stepsize * source)
        return spectrum

    correction = jnp.zeros_like(spec_inflow)
    relaxed = spec_inflow
    defect = jnp.zeros_like(spec_inflow)
    updated_list = []
    defect_list = []
    for interval in range(INTERVALS):
        if interval > 0:
            relaxed = advance(spec_states[interval - 1], spec_forcing[interval - 1])
            correction = coarse * correction + defect
        defect = advance(relaxed, spec_forcing[interval]) - advance(spec_states[interval], spec_forcing[interval])
        updated_list.append(relaxed + correction)
        defect_list.append(defect)
    new_states = jnp.fft.irfftn(jnp.stack(updated_list), s=(GRID, GRID, GRID), axes=(1, 2, 3))
    defects = jnp.fft.irfftn(jnp.stack(defect_list), s=(GRID, GRID, GRID), axes=(1, 2, 3))
    return new_states.astype(jnp.float32), defects.astype(jnp.float32)
```

```python
import math

import jax
import jax.numpy as jnp
from jax import lax
from jax.sharding import PartitionSpec as P

FINE = 8
CHUNKS = 4


def einsum(spec, *operands):
    return jnp.einsum(spec, *operands, precision=lax.Precision.HIGH)


def hartley_table(extent):
    wavenumber = jnp.arange(extent, dtype=jnp.int32)
    product = wavenumber[:, None] * wavenumber[None, :] % extent
    angles = product.astype(jnp.float32) * (2.0 * math.pi / extent)
    return (jnp.cos(angles) + jnp.sin(angles)) * (1.0 / math.sqrt(extent))


def lattice_symbol(wavenumber, extent):
    angles = (wavenumber % extent).astype(jnp.float32) * (2.0 * math.pi / extent)
    return 2.0 - 2.0 * jnp.cos(angles)


def on_device(states, forcing, inflow, timestep):
    planes, extent = states.shape[1], states.shape[2]
    owners = lax.axis_size("space")
    intervals = lax.axis_size("tm")
    place = lax.axis_index("tm")
    rows = planes // CHUNKS
    share = planes // intervals
    hartley = hartley_table(extent)
    stepsize = timestep[0]
    owned = hartley.reshape(owners, planes, extent)

    def swap(blocks):
        return lax.all_to_all(blocks, "space", split_axis=0, concat_axis=0, tiled=True)

    def forward(rows_done, table, after=()):
        blocks = einsum("pzxc,okx->ozpkc", rows_done, table)
        blocks, _ = lax.optimization_barrier((blocks, after))
        sent = swap(blocks)
        return einsum("zpkc,lz->plkc", sent.reshape((extent,) + sent.shape[2:]), hartley)

    rows_states = einsum("pzxy,cy->pzxc", jnp.concatenate([states, forcing], axis=0), hartley)
    rows_inflow = einsum("zxy,cy->zxc", inflow, hartley)[None]

    mine = lax.dynamic_slice_in_dim(owned, place * share, share, 1)
    spec_inflow = lax.all_gather(forward(rows_inflow, mine)[0], "tm")
    spec_inflow = jnp.moveaxis(spec_inflow, 0, 1).reshape(extent, planes, extent)

    full_symbol = lattice_symbol(jnp.arange(extent, dtype=jnp.int32), extent)
    shift_pairs = [(i, i + 1) for i in range(intervals - 1)]
    first = lax.axis_index("space") * planes
    states_back, defects_back, defects, advances, arrivals = [], [], [], [], []
    for chunk in range(CHUNKS):
        lo = chunk * rows
        after = (advances[chunk - 2 : chunk - 1] if chunk >= 2 else [], arrivals[: max(chunk - 2, 0)])
        spectra = forward(rows_states, owned[:, lo : lo + rows], after)
        column = first + lo + jnp.arange(rows, dtype=jnp.int32)
        laplace = (
            full_symbol[:, None, None]
            + lattice_symbol(column, extent)[None, :, None]
            + full_symbol[None, None, :]
        )
        damping = 1.0 / (1.0 + stepsize * laplace)
        coarse = 1.0 / (1.0 + FINE * stepsize * laplace)
        propagator = jnp.ones_like(damping)
        accrued = jnp.zeros_like(damping)
        for repeat in range(FINE):
            propagator = propagator * damping
            accrued = accrued + propagator
        advanced = propagator * spectra[0] + stepsize * accrued * spectra[1]
        advanced, _ = lax.optimization_barrier((advanced, defects[: max(chunk - 1, 0)]))
        arrived = lax.ppermute(advanced, "tm", shift_pairs)
        advances.append(advanced)
        arrivals.append(arrived)
        relaxed = jnp.where(place == 0, spec_inflow[:, lo : lo + rows], arrived)
        defect = propagator * (relaxed - spectra[0])
        defects.append(defect)

        def backward(spectrum):
            got = swap(einsum("lkc,lz->zkc", spectrum, hartley).reshape(owners, planes, rows, extent))
            return einsum("ozkc,cy->zoky", got, hartley)

        defects_back.append(backward(defect))
        gathered = lax.all_gather(defect, "tm")
        correction = jnp.zeros_like(defect)
        for i in range(intervals - 1):
            correction = jnp.where(i < place, coarse * correction + gathered[i], correction)
        states_back.append(backward(relaxed + correction))

    def width_inverse(pieces):
        blocks = jnp.concatenate(pieces, axis=2).reshape(planes, extent, extent)
        return einsum("zky,kx->zxy", blocks, hartley)[None]

    return width_inverse(states_back), width_inverse(defects_back)


def solution(mesh):
    return jax.shard_map(
        on_device,
        mesh=mesh,
        in_specs=(
            P("tm", "space", None, None),
            P("tm", "space", None, None),
            P("space", None, None),
            P(),
        ),
        out_specs=(P("tm", "space", None, None), P("tm", "space", None, None)),
        check_vma=False,
    )
```
